32 devices in a mesh: seq: 16 (over z, y, x), ch: 2 (over core).
Axes of the slice: x: 2, y: 2, z: 4, core: 2. Of those that a mesh axis runs over, the one named last changes fastest.
Arguments:
- tokens: bfloat16 [2048, 8192], P('seq', 'ch'), may hold values from -6 to 6
- query_in: bfloat16 [2048, 8192], P('seq', 'ch'), may hold values from -6 to 6
- key_in: bfloat16 [2048, 8192], P('seq', 'ch'), may hold values from -6 to 6
- proj_in: bfloat16 [8192, 1536], P('ch', 'seq'), may hold values from -0.0625 to 0.0625
- proj_out: bfloat16 [1536, 8192], P('seq', 'ch'), may hold values from -0.15625 to 0.15625
- short_taps: float32 [3, 7, 8192], P(None, None, 'ch'), may hold values from -2.4 to 2.4
- residues: float32 [16, 8192], P(None, 'ch'), may hold values from -1.8 to 1.8
- mode_rates: float32 [16, 8192], P(None, 'ch'), may hold values from 0.00024414062 to 0.03
- skip_gain: float32 [8192], P('ch'), may hold values from -3 to 3
Outputs:
- operator_out: bfloat16 [2048, 8192], P('seq', 'ch')
The draws below stay inside these ranges and needn't reach their ends.
All inputs are finite; a program needn't handle non-finite values.
Results may differ from the reference program's by a relative error of at most 0.0069.
Values may be sent and summed in bfloat16 or wider, within the bound.
No kernel may reach another device: no remote copies, remote signals or barrier semaphores. Data moves between devices by JAX's collectives and lax.ppermute only.
A program may use at most 192 MiB of HBM per device.

```python
import math
import jax
import jax.numpy as jnp
from jax import lax

D = 8192
R = 1536
SHORT = 7
MODES = 16
SEQ = 2048


def steps_of(key, extent, cuts, low, top_value):
    gain, own = 1.0, jax.random.fold_in(key, 6)
    for axis_at, blocks in cuts:
        draws = jnp.exp(jax.random.uniform(jax.random.fold_in(own, axis_at), (blocks,), jnp.float32, low / len(cuts), top_value / len(cuts)))
        gain = gain * jnp.repeat(draws, extent[axis_at] // blocks).reshape([-1 if axis == axis_at else 1 for axis in range(len(extent))])
    return gain


def bell_draw(stream_key, shape, deviation, most, pieces=(), kind=jnp.bfloat16):
    entries = jax.random.normal(stream_key, shape, jnp.float32) * deviation
    if len(pieces) > 0:
        entries = steps_of(stream_key, shape, pieces, -0.22, 0.18) * entries
    return jnp.clip(entries, min=-most, max=most).astype(kind)


def setup_inputs(seed: int = 0) -> dict:
    key_list = jax.random.split(jax.random.key(seed), 10)
    return {
        "tokens": bell_draw(key_list[0], (SEQ, D), 1.0, 6.0, ((0, 16), (1, 2))),
        "query_in": bell_draw(key_list[1], (SEQ, D), 1.0, 6.0, ((0, 16), (1, 2))),
        "key_in": bell_draw(key_list[2], (SEQ, D), 1.0, 6.0, ((0, 16), (1, 2))),
        "proj_in": bell_draw(key_list[3], (D, R), D ** -0.5, 0.0625, ((0, 2), (1, 16))),
        "proj_out": bell_draw(key_list[4], (R, D), R ** -0.5, 0.15625, ((0, 16), (1, 2))),
        "short_taps": bell_draw(key_list[5], (3, SHORT, D), 0.4, 2.4, ((2, 2),), jnp.float32),
        "residues": bell_draw(key_list[6], (MODES, D), 0.3, 1.8, ((1, 2),), jnp.float32),
        "mode_rates": jnp.clip(jnp.exp(math.log(0.03) - 4.8112082 * jax.random.uniform(key_list[7], (MODES, D), jnp.float32) ** steps_of(key_list[7], (MODES, D), ((1, 2),), -0.2, 0.2)), 0.00024414062, 0.03),
        "skip_gain": bell_draw(key_list[8], (D,), 0.5, 3.0, ((0, 2),), jnp.float32),
    }


def causal_short(signal, filter_taps):
    margin_rows = filter_taps.shape[0] - 1
    length = signal.shape[0]
    padded = jnp.pad(signal, ((margin_rows, 0), (0, 0)))
    result = filter_taps[0] * padded[margin_rows:margin_rows + length]
    for offset in range(1, margin_rows + 1):
        result = result + filter_taps[offset] * padded[margin_rows - offset:margin_rows - offset + length]
    return result

def long_block(operands):
    mixed_block, residue_block, rate_block = operands
    positions = jnp.arange(SEQ).astype(jnp.float32)[:, None]
    impulse = jnp.zeros((SEQ, mixed_block.shape[1]), jnp.float32)
    for mode_index in range(MODES):
        impulse = impulse + residue_block[mode_index] * jnp.sqrt(rate_block[mode_index]) * jnp.exp(-rate_block[mode_index] * positions)
    spectrum = jnp.fft.rfft(mixed_block.astype(jnp.float32), n=2 * SEQ, axis=0) * jnp.fft.rfft(impulse, n=2 * SEQ, axis=0)
    return jnp.fft.irfft(spectrum, n=2 * SEQ, axis=0)[:SEQ].astype(jnp.bfloat16)

def reference(tokens, query_in, key_in, proj_in, proj_out, short_taps, residues, mode_rates, skip_gain):
    low_rank = jnp.dot(tokens, proj_in, preferred_element_type=jnp.float32).astype(jnp.bfloat16)
    value_proj = jnp.dot(low_rank, proj_out, preferred_element_type=jnp.float32).astype(jnp.bfloat16)
    query_short = causal_short(query_in.astype(jnp.float32), short_taps[0])
    key_short = causal_short(key_in.astype(jnp.float32), short_taps[1])
    value_short = causal_short(value_proj.astype(jnp.float32), short_taps[2])
    mixed = (key_short * value_short).astype(jnp.bfloat16)
    blocks = D // 128
    mixed_blocks = mixed.reshape(SEQ, blocks, 128).transpose(1, 0, 2)
    residue_blocks = residues.reshape(MODES, blocks, 128).transpose(1, 0, 2)
    rate_blocks = mode_rates.reshape(MODES, blocks, 128).transpose(1, 0, 2)
    convolved = lax.map(long_block, (mixed_blocks, residue_blocks, rate_blocks))
    convolved = convolved.transpose(1, 0, 2).reshape(SEQ, D)
    return (query_short * (convolved.astype(jnp.float32) + skip_gain * mixed.astype(jnp.float32))).astype(jnp.bfloat16)
```

```python
import jax
import jax.numpy as jnp
from jax import lax
from jax.experimental import pallas as pl
from jax.experimental.pallas import tpu as pltpu
from jax.sharding import PartitionSpec as P

LANES = 128
SUBS = 8
VMEM = pl.BlockSpec(memory_space=pltpu.VMEM)
SMEM = pl.BlockSpec(memory_space=pltpu.SMEM)


def tiled_rows(array):
    rows, channels = array.shape
    groups = channels // LANES
    split = array.reshape(rows // SUBS, SUBS, groups, LANES).transpose(0, 2, 1, 3)
    return split.reshape(rows * groups, LANES)


def at_time(ref, tile, step, groups):
    return ref[pl.ds(tile * (groups * SUBS) + step, groups, stride=SUBS), :]


def taps_kernel(signal_ref, taps_ref, out_ref):
    width, groups, _ = taps_ref.shape
    tiles = out_ref.shape[0] // SUBS
    first = tuple(at_time(signal_ref, 0, SUBS - back, groups) for back in range(width - 1, 0, -1))

    def turn(tile, seen):
        for step in range(SUBS):
            seen = seen + (at_time(signal_ref, tile + 1, step, groups),)
            total = taps_ref[0] * seen[-1]
            for back in range(1, width):
                total = total + taps_ref[back] * seen[-1 - back]
            out_ref[tile * SUBS + step] = total
            seen = seen[1:]
        return seen

    lax.fori_loop(0, tiles, turn, first)


def local_kernel(value_ref, key_ref, taps_ref, residues_ref, rates_ref, gain_ref, out_ref, end_ref):
    width, groups, _ = taps_ref.shape
    modes = rates_ref.shape[0]
    tiles = out_ref.shape[0] // SUBS
    decay = [jnp.exp(-rates_ref[n]) for n in range(modes)]
    weight = [residues_ref[n] * jnp.sqrt(rates_ref[n]) for n in range(modes)]
    gain = gain_ref[...]
    taps = [taps_ref[back] for back in range(width)]
    first = tuple(at_time(value_ref, 0, SUBS - back, groups) for back in range(width - 1, 0, -1))
    zero = jnp.zeros_like(gain)

    def turn(tile, carry):
        seen, states = carry
        for step in range(SUBS):
            seen = seen + (at_time(value_ref, tile + 1, step, groups),)
            total = taps[0] * seen[-1]
            for back in range(1, width):
                total = total + taps[back] * seen[-1 - back]
            seen = seen[1:]
            mixed = (total * key_ref[tile * SUBS + step]).astype(jnp.bfloat16).astype(jnp.float32)
            states = tuple(decay[n] * states[n] + mixed for n in range(modes))
            summed = gain * mixed
            for n in range(modes):
                summed = summed + weight[n] * states[n]
            out_ref[tile * SUBS + step] = summed
        return seen, states

    _, states = lax.fori_loop(0, tiles, turn, (first, (zero,) * modes))
    for n in range(modes):
        end_ref[n] = states[n]


def carry_kernel(local_ref, ends_ref, residues_ref, rates_ref, out_ref, tile_ref):
    modes, groups, _ = rates_ref.shape
    rows = local_ref.shape[0]
    decay = [jnp.exp(-rates_ref[n]) for n in range(modes)]
    waves = []
    for n in range(modes):
        rate = rates_ref[n]
        arrived = ends_ref[0, n]
        for far in range(1, ends_ref.shape[0]):
            arrived = arrived + ends_ref[far, n] * jnp.exp(-rate * (far * rows))
        waves.append(residues_ref[n] * jnp.sqrt(rate) * arrived * decay[n])
    pair = 2 * SUBS

    def turn(tile, waves):
        for step in range(pair):
            summed = local_ref[tile * pair + step]
            for n in range(modes):
                summed = summed + waves[n]
            waves = tuple(waves[n] * decay[n] for n in range(modes))
            tile_ref[pl.ds((step // SUBS) * groups * SUBS + step % SUBS, groups, stride=SUBS), :] = summed
        at = pl.ds(pl.multiple_of(tile * pair, pair), pair)
        for group in range(groups):
            upper = tile_ref[pl.ds(group * SUBS, SUBS), :]
            lower = tile_ref[pl.ds((groups + group) * SUBS, SUBS), :]
            both = jnp.concatenate([upper, lower], axis=0)
            out_ref[at, group * LANES : (group + 1) * LANES] = both.astype(out_ref.dtype)
        return waves

    lax.fori_loop(0, rows // pair, turn, tuple(waves))


def final_kernel(inner_ref, query_ref, *refs):
    parts, out_ref = refs[:-1], refs[-1]
    inner = inner_ref[0]
    columns = parts[0].shape[1]
    for far, part in enumerate(parts):
        at = pl.ds(pl.multiple_of((inner ^ far) * columns, columns), columns)
        out_ref[:, at] = (query_ref[:, at] * part[...].astype(jnp.float32)).astype(out_ref.dtype)


def shape_of(shape, dtype=jnp.float32):
    return jax.ShapeDtypeStruct(shape, dtype)


def short_filter(previous, current, filter_taps):
    margin_rows = filter_taps.shape[0] - 1
    length = current.shape[0]
    extended = jnp.concatenate([previous, current], axis=0).astype(jnp.float32)
    skip = previous.shape[0] - margin_rows
    result = filter_taps[0] * extended[skip + margin_rows : skip + margin_rows + length]
    for offset in range(1, margin_rows + 1):
        start = skip + margin_rows - offset
        result = result + filter_taps[offset] * extended[start : start + length]
    return result


def per_device(
    tokens, query_in, key_in, proj_in, proj_out, short_taps, residues, mode_rates, skip_gain
):
    count = lax.axis_size("seq")
    inside = 1 << ((count.bit_length() - 1) // 2)
    outside = count // inside
    mine = lax.axis_index("seq")
    inner, outer = mine % inside, mine // inside
    own_rows, channels = key_in.shape
    block = own_rows * inside
    columns = channels // inside
    groups = columns // LANES
    ranks = proj_out.shape[0]
    ring = [0] + list(range(1, outside, 2)) + [z for z in range(outside - 1, 1, -1) if z % 2 == 0]
    place = [ring.index(z) for z in range(outside)]
    my_place = jnp.asarray(place, jnp.int32)[outer]

    def swap(value, far):
        return lax.ppermute(value, "seq", [(s, s ^ far) for s in range(count)])

    def along(value):
        pairs = [
            (ring[k] * inside + i, ring[(k + 1) % outside] * inside + i)
            for k in range(outside)
            for i in range(inside)
        ]
        return lax.ppermute(value, "seq", pairs)

    def down(value, far, stride):
        step = far * stride
        return lax.ppermute(value, "seq", [(s, s + step) for s in range(count - step)])

    def round_ring(value):
        held = [value]
        for _ in range(outside - 1):
            held.append(along(held[-1]))
        return held

    def columns_for(value, who):
        return lax.dynamic_slice_in_dim(value, who * columns, columns, axis=1)

    def exchange_columns(value):
        return [columns_for(value, inner)] + [
            swap(columns_for(value, inner ^ far), far) for far in range(1, inside)
        ]

    def in_order(parts):
        rows = parts[0].shape[0]
        total = jnp.zeros((rows * inside, parts[0].shape[1]), parts[0].dtype)
        for far, part in enumerate(parts):
            total = lax.dynamic_update_slice_in_dim(total, part, (inner ^ far) * rows, axis=0)
        return total

    first_factor = proj_in.T
    halves = 2 if ranks % 32 == 0 else 1
    cut = ranks // halves
    first_parts = [round_ring(first_factor[h * cut : (h + 1) * cut]) for h in range(halves)]

    second_own = jnp.concatenate(exchange_columns(proj_out), axis=0)
    token_block = in_order([tokens] + [swap(tokens, far) for far in range(1, inside)])
    key_block = in_order(exchange_columns(key_in))
    key_previous = down(key_block[block - SUBS :], 1, inside)
    query_previous = down(query_in[own_rows - SUBS :], 1, 1)

    first_all = jnp.concatenate(
        [first_parts[h][s] for s in range(outside) for h in range(halves)], axis=0
    )
    partial_rank = lax.dot_general(
        token_block, first_all, (((1,), (1,)), ((), ())), preferred_element_type=jnp.float32
    )
    teams = lax.axis_size("ch")
    total_rank = partial_rank
    for far in range(1, teams):
        pairs = [(c, (c + far) % teams) for c in range(teams)]
        total_rank = total_rank + lax.ppermute(partial_rank, "ch", pairs)
    low_own = total_rank.astype(jnp.bfloat16)
    low_all = [low_own] + [swap(low_own, far) for far in range(1, inside)]

    def of_turn(s):
        return jnp.concatenate([part[:, s * ranks : (s + 1) * ranks] for part in low_all], axis=1)

    low_turns = jnp.stack([of_turn(s) for s in range(outside)])

    def reordered(stack, step):
        pick = [(my_place - step(other)) % outside for other in range(outside)]
        return jnp.concatenate([lax.dynamic_slice_in_dim(stack, p, 1, axis=0) for p in pick], axis=0)

    sent = reordered(low_turns[:, block - SUBS :], lambda z: place[z])
    arrived = down(sent, 1, inside)
    owner_of = jnp.asarray(ring, jnp.int32)
    low_halo = jnp.concatenate(
        [
            lax.dynamic_slice_in_dim(arrived, owner_of[(my_place - s) % outside], 1, axis=0)
            for s in range(outside)
        ],
        axis=0,
    )
    low_turns = jnp.concatenate([low_halo, low_turns], axis=1)

    second_parts = round_ring(second_own)
    value = sum(
        jnp.dot(low_turns[s], second_parts[s], preferred_element_type=jnp.float32)
        for s in range(outside)
    )
    value = lax.reduce_precision(value, 8, 7)

    def local(array):
        return lax.dynamic_slice_in_dim(array, inner * columns, columns, axis=array.ndim - 1)

    own_taps = local(short_taps).reshape(short_taps.shape[:2] + (groups, LANES))
    own_residues = local(residues).reshape(-1, groups, LANES)
    own_rates = local(mode_rates).reshape(-1, groups, LANES)
    own_gain = local(skip_gain).reshape(groups, LANES)
    modes = residues.shape[0]

    key_signal = jnp.concatenate([key_previous, key_block], axis=0).astype(jnp.float32)
    key_short = pl.pallas_call(
        taps_kernel,
        out_shape=shape_of((block, groups, LANES)),
        in_specs=[VMEM] * 2,
        out_specs=VMEM,
        name="key_taps",
    )(tiled_rows(key_signal), own_taps[1])
    query_short = short_filter(query_previous, query_in, short_taps[0])

    partial_sum, end_states = pl.pallas_call(
        local_kernel,
        out_shape=(shape_of((block, groups, LANES)), shape_of((modes, groups, LANES))),
        in_specs=[VMEM] * 6,
        out_specs=(VMEM, VMEM),
        name="local_sum",
    )(tiled_rows(value), key_short, own_taps[2], own_residues, own_rates, own_gain)
    ends = jnp.stack([down(end_states, far, inside) for far in range(1, outside)])
    whole_sum = pl.pallas_call(
        carry_kernel,
        out_shape=shape_of((block, columns), jnp.bfloat16),
        in_specs=[VMEM] * 4,
        out_specs=VMEM,
        scratch_shapes=[pltpu.VMEM((2 * SUBS * groups, LANES), jnp.float32)],
        name="carried_sum",
    )(partial_sum, ends, own_residues, own_rates)

    def rows_for(who):
        return lax.dynamic_slice_in_dim(whole_sum, who * own_rows, own_rows, axis=0)

    parts = [rows_for(inner)] + [swap(rows_for(inner ^ far), far) for far in range(1, inside)]
    return pl.pallas_call(
        final_kernel,
        out_shape=shape_of((own_rows, channels), jnp.bfloat16),
        in_specs=[SMEM] + [VMEM] * (1 + inside),
        out_specs=VMEM,
        name="gate",
    )(inner.reshape(1).astype(jnp.int32), query_short, *parts)


def solution(mesh):
    placed = (
        P("seq", "ch"),
        P("seq", "ch"),
        P("seq", "ch"),
        P("ch", "seq"),
        P("seq", "ch"),
        P(None, None, "ch"),
        P(None, "ch"),
        P(None, "ch"),
        P("ch"),
    )
    return jax.shard_map(
        per_device, mesh=mesh, in_specs=placed, out_specs=P("seq", "ch"), check_vma=False
    )
```
